32 devices in a mesh: parts: 2 (over y), seq: 16 (over z, x, core).
Axes of the slice: x: 2, y: 2, z: 4, core: 2. Of those that a mesh axis runs over, the one named last changes fastest.
Arguments:
- queries: bfloat16 [8, 8192], P('parts', 'seq'), parts along dimension 0
- new_kv: bfloat16 [8, 2048], P('parts', 'seq'), parts along dimension 0, may hold values from -6 to 6
- keys: bfloat16 [64, 512, 1024], P(('parts', 'seq')), parts along dimension 0, may hold values from -6 to 6
- values: bfloat16 [64, 512, 1024], P(('parts', 'seq')), parts along dimension 0, may hold values from -6 to 6
- slot_request: int32 [64], P(('parts', 'seq')), parts along dimension 0, may hold values from 0 to 3, as said below
- slot_length: int32 [64], P(('parts', 'seq')), parts along dimension 0, may hold values from 1 to 512
Outputs:
- attended: bfloat16 [8, 8192], P('parts'), parts along dimension 0
The draws below stay inside these ranges and needn't reach their ends.
There are 2 independent parts, one for each index of `parts`. The reference program is written for one: setup_inputs(seed, part) draws one part's arguments, and reference() takes and returns one part's arrays. A program takes and returns all parts, laid end to end along the dimension named above; each array names one. Nothing has to cross between parts.
Inputs may be any that keep to these rules, and one draw needn't show every extreme that they name: `slot_request`: every request number 0 to 3 owns at least one block.
All inputs are finite; a program needn't handle non-finite values.
Results may differ from the reference program's by a relative error of at most 0.0055.
Values may be sent and summed in bfloat16 or wider, within the bound.
A program may use at most 128 MiB of HBM per device.

```python
import jax
import jax.numpy as jnp
from jax import lax

H = 64
KVH = 8
DH = 128
BLOCK = 512
REQ = 4
BLOCKS = 32


def draw_queries(key, part):
    return (1.5 * jax.random.normal(jax.random.fold_in(key, 13), (REQ, H * DH), jnp.float32)).astype(jnp.bfloat16)


def draw_slot_request(key, part):
    first = jax.random.randint(jax.random.fold_in(key, 21), (BLOCKS,), 0, REQ)
    second = jax.random.randint(jax.random.fold_in(key, 22), (BLOCKS,), 0, REQ)
    owners = first * second // REQ
    owners = owners.at[:REQ].set(jnp.arange(REQ, dtype=jnp.int32))
    order = jax.random.permutation(jax.random.fold_in(key, 23), BLOCKS)
    return owners[order].astype(jnp.int32)


def draw_slot_length(key, part):
    choose = jax.random.randint(jax.random.fold_in(key, 31), (BLOCKS,), 0, 3)
    short = jax.random.randint(jax.random.fold_in(key, 32), (BLOCKS,), 1, BLOCK + 1)
    filled = jnp.where(choose == 0, short, BLOCK)
    return filled.at[0].set(BLOCK).astype(jnp.int32)


def shard_levels(rng, extent, cuts, smallest, top_value):
    loudness = 1.0
    for dim, parts in cuts:
        heights = jax.random.uniform(jax.random.fold_in(jax.random.fold_in(rng, 6), dim), (parts,), jnp.float32, smallest / len(cuts), top_value / len(cuts))
        loudness = loudness * jnp.repeat(jnp.exp(heights), extent[dim] // parts).reshape((-1,) + (1,) * (len(extent) - 1 - dim))
    return loudness


def bell_draw(rng, dims, width, most, split=(), held_as=jnp.bfloat16):
    level = shard_levels(rng, dims, split, -0.22, 0.18) if split else 1.0
    array = jax.random.normal(rng, dims, jnp.float32) * width * level
    return jnp.minimum(jnp.maximum(array, -most), most).astype(held_as)


def setup_inputs(seed: int = 0, part: int = 0) -> dict:
    key_list = jax.random.split(jax.random.key(seed), 7)
    part_splits = jax.random.split(jax.random.fold_in(key_list[6], part), 7)
    queries = draw_queries(jax.random.fold_in(jax.random.fold_in(key_list[6], part), 71), part)
    new_kv = bell_draw(part_splits[1], (REQ, 2 * KVH * DH), 1.0, 6.0, ((1, 16),))
    keys = bell_draw(part_splits[2], (BLOCKS, BLOCK, KVH * DH), 1.0, 6.0, ((0, 16),))
    values = bell_draw(part_splits[3], (BLOCKS, BLOCK, KVH * DH), 1.0, 6.0, ((0, 16),))
    slot_request = draw_slot_request(jax.random.fold_in(jax.random.fold_in(key_list[6], part), 71), part)
    slot_length = draw_slot_length(jax.random.fold_in(jax.random.fold_in(key_list[6], part), 71), part)
    return dict(queries=queries, new_kv=new_kv, keys=keys, values=values, slot_request=slot_request, slot_length=slot_length)


very_negative = -1e30


def reference(queries, new_kv, keys, values, slot_request, slot_length):
    requests = queries.shape[0]
    group_size = H // KVH
    score_scale = DH ** -0.5
    query_heads = queries.astype(jnp.float32).reshape(requests, KVH, group_size, DH)
    new_pair = new_kv.astype(jnp.float32).reshape(requests, 2, KVH, DH)
    new_score = jnp.einsum("rkgd,rkd->rkg", query_heads, new_pair[:, 0]) * score_scale
    block_count = keys.shape[0]
    key_tiles = keys.reshape(block_count, BLOCK, KVH, DH)
    value_tiles = values.reshape(block_count, BLOCK, KVH, DH)
    positions = jnp.arange(BLOCK, dtype=jnp.int32)

    def block_scores(key_block, request, length):
        picked = query_heads[request]
        scores = jnp.einsum("kgd,tkd->kgt", picked, key_block.astype(jnp.float32)) * score_scale
        inside = positions < length
        return jnp.where(inside[None, None, :], scores, very_negative)

    def first_pass(items):
        key_block, request, length = items
        return jnp.max(block_scores(key_block, request, length), axis=-1)

    block_top = lax.map(first_pass, (key_tiles, slot_request, slot_length))
    owner = slot_request[:, None] == jnp.arange(requests, dtype=jnp.int32)[None, :]
    request_top = jnp.max(jnp.where(owner[:, :, None, None], block_top[:, None], very_negative), axis=0)
    request_top = jnp.maximum(request_top, new_score)

    def second_pass(items):
        key_block, value_block, request, length = items
        scores = block_scores(key_block, request, length)
        weights = jnp.exp(scores - request_top[request][..., None])
        total = jnp.sum(weights, axis=-1)
        rounded = weights.astype(jnp.bfloat16).astype(jnp.float32)
        numer = jnp.einsum("kgt,tkd->kgd", rounded, value_block.astype(jnp.float32))
        return total, numer

    block_sum, block_out = lax.map(second_pass, (key_tiles, value_tiles, slot_request, slot_length))
    owner_float = owner.astype(jnp.float32)
    total = jnp.einsum("br,bkg->rkg", owner_float, block_sum, precision=lax.Precision.HIGHEST)
    numer = jnp.einsum("br,bkgd->rkgd", owner_float, block_out, precision=lax.Precision.HIGHEST)
    new_weight = jnp.exp(new_score - request_top)
    total = total + new_weight
    rounded_new = new_weight.astype(jnp.bfloat16).astype(jnp.float32)
    numer = numer + rounded_new[..., None] * new_pair[:, 1][:, :, None, :]
    attended = numer / total[..., None]
    return attended.reshape(requests, H * DH).astype(jnp.bfloat16)
```

```python
import functools
import math

import jax
import jax.numpy as jnp
from jax import lax
from jax.experimental import pallas as pl
from jax.experimental.pallas import tpu as pltpu
from jax.sharding import PartitionSpec as P

H = 64
KVH = 8
DH = 128

very_negative = -1e30
LOG2E = math.log2(math.e)
GROUP = H // KVH


def decode_kernel(
    n,
    request_ref,
    length_ref,
    q_ref,
    new_ref,
    keys_ref,
    values_ref,
    out_ref,
    key_buf,
    value_buf,
    q_send,
    q_buf,
    new_buf,
    part_send,
    part_buf,
    stat_send,
    stat_buf,
    out_send,
    load_sem,
    new_sem,
    send_sem,
    recv_sem,
):
    me = lax.axis_index("seq")
    slots, block_len, _ = key_buf.shape
    requests = q_ref.shape[0]
    own = H // n
    rows = own * requests
    span = slots * own
    others = [lax.rem(me + k, n) for k in range(1, n)]

    loads = []
    for s in range(slots):
        load = pltpu.make_async_copy(keys_ref.at[s], key_buf.at[s], load_sem.at[s])
        load.start()
        loads.append(load)
    for s in range(slots):
        load = pltpu.make_async_copy(
            values_ref.at[s], value_buf.at[s], load_sem.at[slots + s]
        )
        load.start()
        loads.append(load)

    barrier = pltpu.get_barrier_semaphore()
    for other in others:
        pl.semaphore_signal(
            barrier, inc=1, device_id={"seq": other}, device_id_type=pl.DeviceIdType.MESH
        )

    mine = q_ref[...].astype(jnp.float32)
    mine = jnp.concatenate([mine[:, c * DH : (c + 1) * DH] for c in range(own)], axis=0)
    q_send[...] = mine.astype(jnp.bfloat16)
    q_buf[me] = mine.astype(jnp.bfloat16)

    pl.semaphore_wait(barrier, n - 1)

    def send(src, dst, phase, other):
        copy = pltpu.make_async_remote_copy(
            src_ref=src,
            dst_ref=dst,
            send_sem=send_sem.at[phase],
            recv_sem=recv_sem.at[phase],
            device_id={"seq": other},
            device_id_type=pl.DeviceIdType.MESH,
        )
        copy.start()

    def drain(buf, sem):
        pltpu.make_async_copy(buf, buf, sem).wait()

    for other in others:
        send(q_send, q_buf.at[me], 0, other)
    half = lax.div(me, KVH)
    head = lax.rem(me, KVH)
    per_kv = n // KVH
    for k in range(per_kv):
        target = head * per_kv + k

        @pl.when(target == me)
        def _():
            pltpu.make_async_copy(new_ref, new_buf.at[half], new_sem.at[half]).start()

        @pl.when(target != me)
        def _():
            pltpu.make_async_remote_copy(
                src_ref=new_ref,
                dst_ref=new_buf.at[half],
                send_sem=new_sem.at[2 + k],
                recv_sem=new_sem.at[half],
                device_id={"seq": target},
                device_id_type=pl.DeviceIdType.MESH,
            ).start()

    others_q = q_buf.at[pl.ds(0, n - 1)]
    drain(others_q, recv_sem.at[0])

    total_rows = n * rows
    pick_row = lax.broadcasted_iota(jnp.int32, (H, total_rows), 0)
    pick_col = lax.broadcasted_iota(jnp.int32, (H, total_rows), 1)
    same_head = lax.div(pick_col, requests) == pick_row
    col_request = lax.rem(pick_col, requests)
    everything = q_buf[...].reshape(total_rows, DH)
    position = lax.broadcasted_iota(jnp.int32, (1, block_len), 1)
    zero = jnp.zeros((GROUP, DH), jnp.bfloat16)
    scale = DH ** (-0.5)

    lane = lax.broadcasted_iota(jnp.int32, (GROUP, DH), 1)
    sub = lax.broadcasted_iota(jnp.int32, (GROUP, DH), 0)
    stat_rows = [None] * KVH
    request_rows = [None] * KVH

    picks = []
    for s in range(slots):
        one_hot = (same_head & (col_request == request_ref[s])).astype(jnp.bfloat16)
        picks.append(jnp.dot(one_hot, everything, preferred_element_type=jnp.float32))

    for s in range(slots):
        loads[s].wait()
        picked = picks[s]
        pieces = []
        for p in range(KVH // 2):
            top_q = picked[2 * p * GROUP : (2 * p + 1) * GROUP].astype(jnp.bfloat16)
            low_q = picked[(2 * p + 1) * GROUP : (2 * p + 2) * GROUP].astype(jnp.bfloat16)
            pair = jnp.concatenate(
                [
                    jnp.concatenate([top_q, zero], axis=1),
                    jnp.concatenate([zero, low_q], axis=1),
                ],
                axis=0,
            )
            pieces.append(
                lax.dot_general(
                    pair,
                    key_buf[s, :, 2 * p * DH : 2 * (p + 1) * DH],
                    (((1,), (1,)), ((), ())),
                    preferred_element_type=jnp.float32,
                )
            )
        scores = jnp.concatenate(pieces, axis=0)
        scores = jnp.where(position < length_ref[s], scores, very_negative)
        top = jnp.max(scores, axis=1, keepdims=True)
        weights = jnp.exp2((scores - top) * (scale * LOG2E))
        total = jnp.sum(weights, axis=1, keepdims=True)
        rounded = weights.astype(jnp.bfloat16)
        inverse = 1.0 / total
        level = top * scale + jnp.log(total)
        loads[slots + s].wait()
        for p in range(KVH // 2):
            wide = jnp.dot(
                rounded[2 * p * GROUP : (2 * p + 2) * GROUP],
                value_buf[s, :, 2 * p * DH : 2 * (p + 1) * DH],
                preferred_element_type=jnp.float32,
            )
            for k in range(2):
                g = 2 * p + k
                block = wide[k * GROUP : (k + 1) * GROUP, k * DH : (k + 1) * DH]
                block = block * inverse[g * GROUP : (g + 1) * GROUP]
                for d in range(GROUP // own):
                    part_send[g * (GROUP // own) + d, s * own : (s + 1) * own, :] = block[
                        d * own : (d + 1) * own
                    ].astype(jnp.bfloat16)
        here = lane == me * span + s * own + lax.rem(sub, own)
        for g in range(KVH):
            level_g = jnp.where(here, level[g * GROUP : (g + 1) * GROUP], 0.0)
            stat_rows[g] = level_g if s == 0 else stat_rows[g] + level_g
        owner = jnp.where(here, request_ref[s].astype(jnp.float32), 0.0)
        owners = owner if s == 0 else owners + owner

    owners = jnp.sum(owners[:own], axis=0, keepdims=True)
    for g in range(KVH):
        for d in range(GROUP // own):
            row = jnp.sum(stat_rows[g][d * own : (d + 1) * own], axis=0, keepdims=True)
            stat_send[g * (GROUP // own) + d] = jnp.concatenate([row, owners], axis=0)

    stat_buf[me] = stat_send[me]
    part_buf[me] = part_send[me]
    for other in others:
        send(stat_send.at[other], stat_buf.at[me], 1, other)
        send(part_send.at[other], part_buf.at[me], 2, other)

    drain(new_buf.at[0], new_sem.at[0])
    drain(new_buf.at[1], new_sem.at[1])
    new_key = jnp.concatenate([new_buf[0].astype(jnp.float32)] * own, axis=0)
    new_value = jnp.concatenate([new_buf[1].astype(jnp.float32)] * own, axis=0)
    new_score = jnp.sum(mine * new_key, axis=1, keepdims=True) * scale

    drain(stat_buf.at[pl.ds(0, n - 1)], recv_sem.at[1])
    stats = jnp.sum(stat_buf[...], axis=0)
    levels = stats[0:1]
    slot_owner = stats[1:2]
    row_id = lax.broadcasted_iota(jnp.int32, (rows, n * span), 0)
    col_id = lax.broadcasted_iota(jnp.int32, (rows, n * span), 1)
    same = lax.rem(col_id, own) == lax.div(row_id, requests)
    belongs = same & (slot_owner == lax.rem(row_id, requests).astype(jnp.float32))
    peak = jnp.max(jnp.where(belongs, levels, very_negative), axis=1, keepdims=True)
    peak = jnp.maximum(peak, new_score)
    mix = jnp.where(belongs, jnp.exp2((levels - peak) * LOG2E), 0.0)
    new_weight = jnp.exp2((new_score - peak) * LOG2E)
    denom = jnp.sum(mix, axis=1, keepdims=True) + new_weight
    mix = mix * (1.0 / denom)
    new_weight = new_weight * (1.0 / denom)
    mix_high = mix.astype(jnp.bfloat16)
    mix_low = (mix - mix_high.astype(jnp.float32)).astype(jnp.bfloat16)

    drain(part_buf.at[pl.ds(0, n - 1)], recv_sem.at[2])
    parts = part_buf[...].reshape(n * span, DH)
    result = jnp.dot(
        jnp.concatenate([mix_high, mix_low], axis=0), parts, preferred_element_type=jnp.float32
    )
    result = result[:rows] + result[rows:] + new_weight * new_value
    result = jnp.concatenate(
        [result[c * requests : (c + 1) * requests] for c in range(own)], axis=1
    ).astype(jnp.bfloat16)
    out_send[...] = result
    columns = pl.ds(pl.multiple_of(me * own * DH, own * DH), own * DH)
    out_ref[:, columns] = result
    for other in others:
        send(out_send, out_ref.at[:, columns], 3, other)

    drain(q_buf.at[pl.ds(0, n - 1)], send_sem.at[0])
    drain(stat_buf.at[pl.ds(0, n - 1)], send_sem.at[1])
    drain(part_buf.at[pl.ds(0, n - 1)], send_sem.at[2])
    for k in range(per_kv):

        @pl.when(head * per_kv + k != me)
        def _():
            drain(new_buf.at[0], new_sem.at[2 + k])

    rest = out_ref.at[:, pl.ds(0, (n - 1) * own * DH)]
    drain(rest, send_sem.at[3])
    drain(rest, recv_sem.at[3])


def one_kernel(n, queries, new_kv, keys, values, slot_request, slot_length):
    requests = queries.shape[0]
    slots, block_len, width = keys.shape
    own = H // n
    span = slots * own
    bf16, f32 = jnp.bfloat16, jnp.float32
    smem = pl.BlockSpec(memory_space=pltpu.SMEM)
    vmem = pl.BlockSpec(memory_space=pltpu.VMEM)
    hbm = pl.BlockSpec(memory_space=pl.ANY)
    return pl.pallas_call(
        functools.partial(decode_kernel, n),
        out_shape=jax.ShapeDtypeStruct((requests, H * DH), bf16),
        in_specs=[smem, smem, vmem, vmem, hbm, hbm],
        out_specs=vmem,
        scratch_shapes=[
            pltpu.VMEM((slots, block_len, width), bf16),
            pltpu.VMEM((slots, block_len, width), bf16),
            pltpu.VMEM((own * requests, DH), bf16),
            pltpu.VMEM((n, own * requests, DH), bf16),
            pltpu.VMEM((2, requests, DH), bf16),
            pltpu.VMEM((n, span, DH), bf16),
            pltpu.VMEM((n, span, DH), bf16),
            pltpu.VMEM((n, 2, n * span), f32),
            pltpu.VMEM((n, 2, n * span), f32),
            pltpu.VMEM((requests, own * DH), bf16),
            pltpu.SemaphoreType.DMA((2 * slots,)),
            pltpu.SemaphoreType.DMA((2 + n // KVH,)),
            pltpu.SemaphoreType.DMA((4,)),
            pltpu.SemaphoreType.DMA((4,)),
        ],
        compiler_params=pltpu.CompilerParams(collective_id=0, has_side_effects=True),
    )(slot_request, slot_length, queries, new_kv, keys, values)


def joined(x, axis, combine):
    everything = jax.tree.map(lambda part: lax.all_gather(part, axis), x)
    leading = jax.tree.map(lambda part: part[0], everything)

    def turn(k, so_far):
        return combine(so_far, jax.tree.map(lambda part: part[k], everything))

    return lax.fori_loop(1, lax.axis_size(axis), turn, leading)


def combine_parts(first, second):
    top_first, sum_first, out_first = first
    top_second, sum_second, out_second = second
    peak = jnp.maximum(top_first, top_second)
    weight_first = jnp.exp(top_first - peak)
    weight_second = jnp.exp(top_second - peak)
    summed = sum_first * weight_first + sum_second * weight_second
    outputs = out_first * weight_first[..., None] + out_second * weight_second[..., None]
    return (peak, summed, outputs)


def gathered(queries, new_kv, keys, values, slot_request, slot_length):
    all_queries, all_new = (
        lax.all_gather(queries, "seq", axis=1, tiled=True),
        lax.all_gather(new_kv, "seq", axis=1, tiled=True),
    )
    requests = all_queries.shape[0]
    group_size = H // KVH
    score_scale = DH ** (-0.5)
    query_heads = all_queries.reshape(requests, KVH, group_size, DH)
    slot_count = keys.shape[0]
    block_len = keys.shape[1]
    owner = slot_request[:, None] == jnp.arange(requests, dtype=jnp.int32)[None, :]
    picked = jnp.einsum(
        "sr,rkgd->skgd", owner.astype(jnp.bfloat16), query_heads, preferred_element_type=jnp.float32
    ).astype(jnp.bfloat16)
    key_tiles = keys.reshape(slot_count, block_len, KVH, DH)
    value_tiles = values.reshape(slot_count, block_len, KVH, DH)
    scores = (
        jnp.einsum("skgd,stkd->skgt", picked, key_tiles, preferred_element_type=jnp.float32)
        * score_scale
    )
    inside = jnp.arange(block_len, dtype=jnp.int32)[None, :] < slot_length[:, None]
    scores = jnp.where(inside[:, None, None, :], scores, very_negative)
    slot_top = jnp.max(scores, axis=-1)
    weights = jnp.exp(scores - slot_top[..., None])
    slot_sum = jnp.sum(weights, axis=-1)
    slot_out = jnp.einsum(
        "skgt,stkd->skgd",
        weights.astype(jnp.bfloat16),
        value_tiles,
        preferred_element_type=jnp.float32,
    )
    owner_wide = owner[:, :, None, None]
    dense_top = jnp.max(jnp.where(owner_wide, slot_top[:, None], very_negative), axis=0)
    factor = jnp.where(owner_wide, jnp.exp(slot_top[:, None] - dense_top[None]), 0.0)
    dense_sum = jnp.sum(factor * slot_sum[:, None], axis=0)
    dense_out = jnp.einsum("srkg,skgd->rkgd", factor, slot_out, precision=lax.Precision.HIGHEST)
    total_top, total_sum, total_out = joined(
        (dense_top, dense_sum, dense_out), "seq", combine_parts
    )
    new_pair = all_new.astype(jnp.float32).reshape(requests, 2, KVH, DH)
    new_score = (
        jnp.einsum("rkgd,rkd->rkg", query_heads.astype(jnp.float32), new_pair[:, 0]) * score_scale
    )
    peak = jnp.maximum(total_top, new_score)
    old_weight = jnp.exp(total_top - peak)
    new_weight = jnp.exp(new_score - peak)
    rounded_new = new_weight.astype(jnp.bfloat16).astype(jnp.float32)
    numer = (
        total_out * old_weight[..., None] + rounded_new[..., None] * new_pair[:, 1][:, :, None, :]
    )
    denom = total_sum * old_weight + new_weight
    attended = numer / denom[..., None]
    return attended.reshape(requests, H * DH).astype(jnp.bfloat16)


def shards(n, queries, new_kv, keys, values, slot_request, slot_length):
    whole_heads = n == 2 * KVH and n * keys.shape[0] * (H // n) == DH
    if whole_heads:
        return one_kernel(n, queries, new_kv, keys, values, slot_request, slot_length)
    return gathered(queries, new_kv, keys, values, slot_request, slot_length)


def solution(mesh):
    placed = (
        P("parts", "seq"),
        P("parts", "seq"),
        P(("parts", "seq"), None, None),
        P(("parts", "seq"), None, None),
        P(("parts", "seq")),
        P(("parts", "seq")),
    )
    return jax.shard_map(
        functools.partial(shards, mesh.shape["seq"]),
        mesh=mesh,
        in_specs=placed,
        out_specs=P("parts", None),
        check_vma=False,
    )
```

```python
import functools
import math

import jax
import jax.numpy as jnp
from jax import lax
from jax.experimental import pallas as pl
from jax.experimental.pallas import tpu as pltpu
from jax.sharding import PartitionSpec as P

H = 64
KVH = 8
DH = 128

very_negative = -1e30
LOG2E = math.log2(math.e)
GROUP = H // KVH


def decode_kernel(
    n,
    request_hbm,
    length_hbm,
    q_hbm,
    new_hbm,
    keys_ref,
    values_ref,
    out_ref,
    q_ref,
    new_ref,
    request_ref,
    length_ref,
    small_sem,
    key_buf,
    value_buf,
    q_send,
    q_buf,
    new_buf,
    part_send,
    part_buf,
    stat_send,
    stat_buf,
    out_send,
    load_sem,
    new_sem,
    send_sem,
    recv_sem,
):
    me = lax.axis_index("seq")
    slots, block_len, _ = key_buf.shape
    requests = q_ref.shape[0]
    own = H // n
    rows = own * requests
    span = slots * own
    others = [lax.rem(me + k, n) for k in range(1, n)]

    barrier = pltpu.get_barrier_semaphore()
    for other in others:
        pl.semaphore_signal(
            barrier, inc=1, device_id={"seq": other}, device_id_type=pl.DeviceIdType.MESH
        )

    small = []
    for k, (src, dst) in enumerate(
        [(q_hbm, q_ref), (new_hbm, new_ref), (request_hbm, request_ref), (length_hbm, length_ref)]
    ):
        copy = pltpu.make_async_copy(src, dst, small_sem.at[k])
        copy.start()
        small.append(copy)
    loads = []
    for s in range(slots):
        load = pltpu.make_async_copy(keys_ref.at[s], key_buf.at[s], load_sem.at[s])
        load.start()
        loads.append(load)
    for s in range(slots):
        load = pltpu.make_async_copy(
            values_ref.at[s], value_buf.at[s], load_sem.at[slots + s]
        )
        load.start()
        loads.append(load)

    small[0].wait()
    mine = q_ref[...].astype(jnp.float32)
    mine = jnp.concatenate([mine[:, c * DH : (c + 1) * DH] for c in range(own)], axis=0)
    q_send[...] = mine.astype(jnp.bfloat16)
    q_buf[me] = mine.astype(jnp.bfloat16)

    pl.semaphore_wait(barrier, n - 1)

    def send(src, dst, phase, other):
        copy = pltpu.make_async_remote_copy(
            src_ref=src,
            dst_ref=dst,
            send_sem=send_sem.at[phase],
            recv_sem=recv_sem.at[phase],
            device_id={"seq": other},
            device_id_type=pl.DeviceIdType.MESH,
        )
        copy.start()

    def drain(buf, sem):
        pltpu.make_async_copy(buf, buf, sem).wait()

    for other in others:
        send(q_send, q_buf.at[me], 0, other)
    for copy in small[1:]:
        copy.wait()
    half = lax.div(me, KVH)
    head = lax.rem(me, KVH)
    per_kv = n // KVH
    for k in range(per_kv):
        target = head * per_kv + k

        @pl.when(target == me)
        def _():
            pltpu.make_async_copy(new_ref, new_buf.at[half], new_sem.at[half]).start()

        @pl.when(target != me)
        def _():
            pltpu.make_async_remote_copy(
                src_ref=new_ref,
                dst_ref=new_buf.at[half],
                send_sem=new_sem.at[2 + k],
                recv_sem=new_sem.at[half],
                device_id={"seq": target},
                device_id_type=pl.DeviceIdType.MESH,
            ).start()

    others_q = q_buf.at[pl.ds(0, n - 1)]
    drain(others_q, recv_sem.at[0])

    total_rows = n * rows
    pick_row = lax.broadcasted_iota(jnp.int32, (H, total_rows), 0)
    pick_col = lax.broadcasted_iota(jnp.int32, (H, total_rows), 1)
    same_head = lax.div(pick_col, requests) == pick_row
    col_request = lax.rem(pick_col, requests)
    everything = q_buf[...].reshape(total_rows, DH)
    position = lax.broadcasted_iota(jnp.int32, (1, block_len), 1)
    zero = jnp.zeros((GROUP, DH), jnp.bfloat16)
    scale = DH ** (-0.5)

    lane = lax.broadcasted_iota(jnp.int32, (GROUP, DH), 1)
    sub = lax.broadcasted_iota(jnp.int32, (GROUP, DH), 0)
    stat_rows = [None] * KVH
    request_rows = [None] * KVH

    picks = []
    for s in range(slots):
        one_hot = (same_head & (col_request == request_ref[s])).astype(jnp.bfloat16)
        picks.append(jnp.dot(one_hot, everything, preferred_element_type=jnp.float32))

    for s in range(slots):
        loads[s].wait()
        picked = picks[s]
        pieces = []
        for p in range(KVH // 2):
            top_q = picked[2 * p * GROUP : (2 * p + 1) * GROUP].astype(jnp.bfloat16)
            low_q = picked[(2 * p + 1) * GROUP : (2 * p + 2) * GROUP].astype(jnp.bfloat16)
            pair = jnp.concatenate(
                [
                    jnp.concatenate([top_q, zero], axis=1),
                    jnp.concatenate([zero, low_q], axis=1),
                ],
                axis=0,
            )
            pieces.append(
                lax.dot_general(
                    pair,
                    key_buf[s, :, 2 * p * DH : 2 * (p + 1) * DH],
                    (((1,), (1,)), ((), ())),
                    preferred_element_type=jnp.float32,
                )
            )
        scores = jnp.concatenate(pieces, axis=0)
        scores = jnp.where(position < length_ref[s], scores, very_negative)
        top = jnp.max(scores, axis=1, keepdims=True)
        weights = jnp.exp2((scores - top) * (scale * LOG2E))
        total = jnp.sum(weights, axis=1, keepdims=True)
        rounded = weights.astype(jnp.bfloat16)
        inverse = 1.0 / total
        level = top * scale + jnp.log(total)
        loads[slots + s].wait()
        for p in range(KVH // 2):
            wide = jnp.dot(
                rounded[2 * p * GROUP : (2 * p + 2) * GROUP],
                value_buf[s, :, 2 * p * DH : 2 * (p + 1) * DH],
                preferred_element_type=jnp.float32,
            )
            for k in range(2):
                g = 2 * p + k
                block = wide[k * GROUP : (k + 1) * GROUP, k * DH : (k + 1) * DH]
                block = block * inverse[g * GROUP : (g + 1) * GROUP]
                for d in range(GROUP // own):
                    part_send[g * (GROUP // own) + d, s * own : (s + 1) * own, :] = block[
                        d * own : (d + 1) * own
                    ].astype(jnp.bfloat16)
        here = lane == me * span + s * own + lax.rem(sub, own)
        for g in range(KVH):
            level_g = jnp.where(here, level[g * GROUP : (g + 1) * GROUP], 0.0)
            stat_rows[g] = level_g if s == 0 else stat_rows[g] + level_g
        owner = jnp.where(here, request_ref[s].astype(jnp.float32), 0.0)
        owners = owner if s == 0 else owners + owner

    owners = jnp.sum(owners[:own], axis=0, keepdims=True)
    for g in range(KVH):
        for d in range(GROUP // own):
            row = jnp.sum(stat_rows[g][d * own : (d + 1) * own], axis=0, keepdims=True)
            stat_send[g * (GROUP // own) + d] = jnp.concatenate([row, owners], axis=0)

    stat_buf[me] = stat_send[me]
    part_buf[me] = part_send[me]
    for other in others:
        send(stat_send.at[other], stat_buf.at[me], 1, other)
        send(part_send.at[other], part_buf.at[me], 2, other)

    drain(new_buf.at[0], new_sem.at[0])
    drain(new_buf.at[1], new_sem.at[1])
    new_key = jnp.concatenate([new_buf[0].astype(jnp.float32)] * own, axis=0)
    new_value = jnp.concatenate([new_buf[1].astype(jnp.float32)] * own, axis=0)
    new_score = jnp.sum(mine * new_key, axis=1, keepdims=True) * scale

    drain(stat_buf.at[pl.ds(0, n - 1)], recv_sem.at[1])
    stats = jnp.sum(stat_buf[...], axis=0)
    levels = stats[0:1]
    slot_owner = stats[1:2]
    row_id = lax.broadcasted_iota(jnp.int32, (rows, n * span), 0)
    col_id = lax.broadcasted_iota(jnp.int32, (rows, n * span), 1)
    same = lax.rem(col_id, own) == lax.div(row_id, requests)
    belongs = same & (slot_owner == lax.rem(row_id, requests).astype(jnp.float32))
    peak = jnp.max(jnp.where(belongs, levels, very_negative), axis=1, keepdims=True)
    peak = jnp.maximum(peak, new_score)
    mix = jnp.where(belongs, jnp.exp2((levels - peak) * LOG2E), 0.0)
    new_weight = jnp.exp2((new_score - peak) * LOG2E)
    denom = jnp.sum(mix, axis=1, keepdims=True) + new_weight
    mix = mix * (1.0 / denom)
    new_weight = new_weight * (1.0 / denom)
    mix_high = mix.astype(jnp.bfloat16)
    mix_low = (mix - mix_high.astype(jnp.float32)).astype(jnp.bfloat16)

    drain(part_buf.at[pl.ds(0, n - 1)], recv_sem.at[2])
    parts = part_buf[...].reshape(n * span, DH)
    result = jnp.dot(
        jnp.concatenate([mix_high, mix_low], axis=0), parts, preferred_element_type=jnp.float32
    )
    result = result[:rows] + result[rows:] + new_weight * new_value
    result = jnp.concatenate(
        [result[c * requests : (c + 1) * requests] for c in range(own)], axis=1
    ).astype(jnp.bfloat16)
    out_send[...] = result
    columns = pl.ds(pl.multiple_of(me * own * DH, own * DH), own * DH)
    out_ref[:, columns] = result
    for other in others:
        send(out_send, out_ref.at[:, columns], 3, other)

    drain(q_buf.at[pl.ds(0, n - 1)], send_sem.at[0])
    drain(stat_buf.at[pl.ds(0, n - 1)], send_sem.at[1])
    drain(part_buf.at[pl.ds(0, n - 1)], send_sem.at[2])
    for k in range(per_kv):

        @pl.when(head * per_kv + k != me)
        def _():
            drain(new_buf.at[0], new_sem.at[2 + k])

    rest = out_ref.at[:, pl.ds(0, (n - 1) * own * DH)]
    drain(rest, send_sem.at[3])
    drain(rest, recv_sem.at[3])


def one_kernel(n, queries, new_kv, keys, values, slot_request, slot_length):
    requests = queries.shape[0]
    slots, block_len, width = keys.shape
    own = H // n
    span = slots * own
    bf16, f32 = jnp.bfloat16, jnp.float32
    vmem = pl.BlockSpec(memory_space=pltpu.VMEM)
    hbm = pl.BlockSpec(memory_space=pl.ANY)
    return pl.pallas_call(
        functools.partial(decode_kernel, n),
        out_shape=jax.ShapeDtypeStruct((requests, H * DH), bf16),
        in_specs=[hbm] * 6,
        out_specs=vmem,
        scratch_shapes=[
            pltpu.VMEM(queries.shape, bf16),
            pltpu.VMEM(new_kv.shape, bf16),
            pltpu.SMEM(slot_request.shape, jnp.int32),
            pltpu.SMEM(slot_length.shape, jnp.int32),
            pltpu.SemaphoreType.DMA((4,)),
            pltpu.VMEM((slots, block_len, width), bf16),
            pltpu.VMEM((slots, block_len, width), bf16),
            pltpu.VMEM((own * requests, DH), bf16),
            pltpu.VMEM((n, own * requests, DH), bf16),
            pltpu.VMEM((2, requests, DH), bf16),
            pltpu.VMEM((n, span, DH), bf16),
            pltpu.VMEM((n, span, DH), bf16),
            pltpu.VMEM((n, 2, n * span), f32),
            pltpu.VMEM((n, 2, n * span), f32),
            pltpu.VMEM((requests, own * DH), bf16),
            pltpu.SemaphoreType.DMA((2 * slots,)),
            pltpu.SemaphoreType.DMA((2 + n // KVH,)),
            pltpu.SemaphoreType.DMA((4,)),
            pltpu.SemaphoreType.DMA((4,)),
        ],
        compiler_params=pltpu.CompilerParams(collective_id=0, has_side_effects=True),
    )(slot_request, slot_length, queries, new_kv, keys, values)


def joined(x, axis, combine):
    everything = jax.tree.map(lambda part: lax.all_gather(part, axis), x)
    leading = jax.tree.map(lambda part: part[0], everything)

    def turn(k, so_far):
        return combine(so_far, jax.tree.map(lambda part: part[k], everything))

    return lax.fori_loop(1, lax.axis_size(axis), turn, leading)


def combine_parts(first, second):
    top_first, sum_first, out_first = first
    top_second, sum_second, out_second = second
    peak = jnp.maximum(top_first, top_second)
    weight_first = jnp.exp(top_first - peak)
    weight_second = jnp.exp(top_second - peak)
    summed = sum_first * weight_first + sum_second * weight_second
    outputs = out_first * weight_first[..., None] + out_second * weight_second[..., None]
    return (peak, summed, outputs)


def gathered(queries, new_kv, keys, values, slot_request, slot_length):
    all_queries, all_new = (
        lax.all_gather(queries, "seq", axis=1, tiled=True),
        lax.all_gather(new_kv, "seq", axis=1, tiled=True),
    )
    requests = all_queries.shape[0]
    group_size = H // KVH
    score_scale = DH ** (-0.5)
    query_heads = all_queries.reshape(requests, KVH, group_size, DH)
    slot_count = keys.shape[0]
    block_len = keys.shape[1]
    owner = slot_request[:, None] == jnp.arange(requests, dtype=jnp.int32)[None, :]
    picked = jnp.einsum(
        "sr,rkgd->skgd", owner.astype(jnp.bfloat16), query_heads, preferred_element_type=jnp.float32
    ).astype(jnp.bfloat16)
    key_tiles = keys.reshape(slot_count, block_len, KVH, DH)
    value_tiles = values.reshape(slot_count, block_len, KVH, DH)
    scores = (
        jnp.einsum("skgd,stkd->skgt", picked, key_tiles, preferred_element_type=jnp.float32)
        * score_scale
    )
    inside = jnp.arange(block_len, dtype=jnp.int32)[None, :] < slot_length[:, None]
    scores = jnp.where(inside[:, None, None, :], scores, very_negative)
    slot_top = jnp.max(scores, axis=-1)
    weights = jnp.exp(scores - slot_top[..., None])
    slot_sum = jnp.sum(weights, axis=-1)
    slot_out = jnp.einsum(
        "skgt,stkd->skgd",
        weights.astype(jnp.bfloat16),
        value_tiles,
        preferred_element_type=jnp.float32,
    )
    owner_wide = owner[:, :, None, None]
    dense_top = jnp.max(jnp.where(owner_wide, slot_top[:, None], very_negative), axis=0)
    factor = jnp.where(owner_wide, jnp.exp(slot_top[:, None] - dense_top[None]), 0.0)
    dense_sum = jnp.sum(factor * slot_sum[:, None], axis=0)
    dense_out = jnp.einsum("srkg,skgd->rkgd", factor, slot_out, precision=lax.Precision.HIGHEST)
    total_top, total_sum, total_out = joined(
        (dense_top, dense_sum, dense_out), "seq", combine_parts
    )
    new_pair = all_new.astype(jnp.float32).reshape(requests, 2, KVH, DH)
    new_score = (
        jnp.einsum("rkgd,rkd->rkg", query_heads.astype(jnp.float32), new_pair[:, 0]) * score_scale
    )
    peak = jnp.maximum(total_top, new_score)
    old_weight = jnp.exp(total_top - peak)
    new_weight = jnp.exp(new_score - peak)
    rounded_new = new_weight.astype(jnp.bfloat16).astype(jnp.float32)
    numer = (
        total_out * old_weight[..., None] + rounded_new[..., None] * new_pair[:, 1][:, :, None, :]
    )
    denom = total_sum * old_weight + new_weight
    attended = numer / denom[..., None]
    return attended.reshape(requests, H * DH).astype(jnp.bfloat16)


def shards(n, queries, new_kv, keys, values, slot_request, slot_length):
    whole_heads = n == 2 * KVH and n * keys.shape[0] * (H // n) == DH
    if whole_heads:
        return one_kernel(n, queries, new_kv, keys, values, slot_request, slot_length)
    return gathered(queries, new_kv, keys, values, slot_request, slot_length)


def solution(mesh):
    placed = (
        P("parts", "seq"),
        P("parts", "seq"),
        P(("parts", "seq"), None, None),
        P(("parts", "seq"), None, None),
        P(("parts", "seq")),
        P(("parts", "seq")),
    )
    return jax.shard_map(
        functools.partial(shards, mesh.shape["seq"]),
        mesh=mesh,
        in_specs=placed,
        out_specs=P("parts", None),
        check_vma=False,
    )
```

```python
import functools
import math

import jax
import jax.numpy as jnp
from jax import lax
from jax.experimental import pallas as pl
from jax.experimental.pallas import tpu as pltpu
from jax.sharding import PartitionSpec as P

H = 64
KVH = 8
DH = 128

very_negative = -1e30
LOG2E = math.log2(math.e)
GROUP = H // KVH


def decode_kernel(
    n,
    request_hbm,
    length_hbm,
    q_hbm,
    new_hbm,
    keys_ref,
    values_ref,
    out_ref,
    q_ref,
    new_ref,
    request_ref,
    length_ref,
    small_sem,
    key_buf,
    value_buf,
    q_send,
    q_buf,
    new_buf,
    part_send,
    part_buf,
    stat_send,
    stat_buf,
    out_send,
    load_sem,
    new_sem,
    send_sem,
    recv_sem,
):
    me = lax.axis_index("seq")
    slots, block_len, _ = key_buf.shape
    requests = q_ref.shape[0]
    own = H // n
    rows = own * requests
    span = slots * own
    others = [lax.rem(me + k, n) for k in range(1, n)]

    barrier = pltpu.get_barrier_semaphore()
    for other in others:
        pl.semaphore_signal(
            barrier, inc=1, device_id={"seq": other}, device_id_type=pl.DeviceIdType.MESH
        )

    small = []
    for k, (src, dst) in enumerate(
        [(q_hbm, q_ref), (new_hbm, new_ref), (request_hbm, request_ref), (length_hbm, length_ref)]
    ):
        copy = pltpu.make_async_copy(src, dst, small_sem.at[k])
        copy.start()
        small.append(copy)
    loads = []
    for s in range(slots):
        load = pltpu.make_async_copy(keys_ref.at[s], key_buf.at[s], load_sem.at[s])
        load.start()
        loads.append(load)
    for s in range(slots):
        load = pltpu.make_async_copy(
            values_ref.at[s], value_buf.at[s], load_sem.at[slots + s]
        )
        load.start()
        loads.append(load)

    small[0].wait()
    mine = q_ref[...].astype(jnp.float32)
    mine = jnp.concatenate([mine[:, c * DH : (c + 1) * DH] for c in range(own)], axis=0)
    q_send[...] = mine.astype(jnp.bfloat16)
    q_buf[me] = mine.astype(jnp.bfloat16)

    pl.semaphore_wait(barrier, n - 1)

    def send(src, dst, phase, other):
        copy = pltpu.make_async_remote_copy(
            src_ref=src,
            dst_ref=dst,
            send_sem=send_sem.at[phase],
            recv_sem=recv_sem.at[phase],
            device_id={"seq": other},
            device_id_type=pl.DeviceIdType.MESH,
        )
        copy.start()

    def drain(buf, sem):
        pltpu.make_async_copy(buf, buf, sem).wait()

    for other in others:
        send(q_send, q_buf.at[me], 0, other)
    for copy in small[1:]:
        copy.wait()
    half = lax.div(me, KVH)
    head = lax.rem(me, KVH)
    per_kv = n // KVH
    for k in range(per_kv):
        target = head * per_kv + k

        @pl.when(target == me)
        def _():
            pltpu.make_async_copy(new_ref, new_buf.at[half], new_sem.at[half]).start()

        @pl.when(target != me)
        def _():
            pltpu.make_async_remote_copy(
                src_ref=new_ref,
                dst_ref=new_buf.at[half],
                send_sem=new_sem.at[2 + k],
                recv_sem=new_sem.at[half],
                device_id={"seq": target},
                device_id_type=pl.DeviceIdType.MESH,
            ).start()

    others_q = q_buf.at[pl.ds(0, n - 1)]
    drain(others_q, recv_sem.at[0])

    total_rows = n * rows
    pick_row = lax.broadcasted_iota(jnp.int32, (H, total_rows), 0)
    pick_col = lax.broadcasted_iota(jnp.int32, (H, total_rows), 1)
    same_head = lax.div(pick_col, requests) == pick_row
    col_request = lax.rem(pick_col, requests)
    everything = q_buf[...].reshape(total_rows, DH)
    position = lax.broadcasted_iota(jnp.int32, (1, block_len), 1)
    zero = jnp.zeros((GROUP, DH), jnp.bfloat16)
    scale = DH ** (-0.5)

    lane = lax.broadcasted_iota(jnp.int32, (GROUP, DH), 1)
    sub = lax.broadcasted_iota(jnp.int32, (GROUP, DH), 0)
    stat_rows = [None] * KVH
    request_rows = [None] * KVH

    picks = []
    for s in range(slots):
        one_hot = (same_head & (col_request == request_ref[s])).astype(jnp.bfloat16)
        picks.append(jnp.dot(one_hot, everything, preferred_element_type=jnp.float32))

    for s in range(slots):
        loads[s].wait()
        picked = picks[s]
        pieces = []
        for p in range(KVH // 2):
            top_q = picked[2 * p * GROUP : (2 * p + 1) * GROUP].astype(jnp.bfloat16)
            low_q = picked[(2 * p + 1) * GROUP : (2 * p + 2) * GROUP].astype(jnp.bfloat16)
            pair = jnp.concatenate(
                [
                    jnp.concatenate([top_q, zero], axis=1),
                    jnp.concatenate([zero, low_q], axis=1),
                ],
                axis=0,
            )
            pieces.append(
                lax.dot_general(
                    pair,
                    key_buf[s, :, 2 * p * DH : 2 * (p + 1) * DH],
                    (((1,), (1,)), ((), ())),
                    preferred_element_type=jnp.float32,
                )
            )
        scores = jnp.concatenate(pieces, axis=0)
        scores = jnp.where(position < length_ref[s], scores, very_negative)
        top = jnp.max(scores, axis=1, keepdims=True)
        weights = jnp.exp2((scores - top) * (scale * LOG2E))
        total = jnp.sum(weights, axis=1, keepdims=True)
        rounded = weights.astype(jnp.bfloat16)
        inverse = 1.0 / total
        level = top * scale + jnp.log(total)
        loads[slots + s].wait()
        for p in range(KVH // 2):
            wide = jnp.dot(
                rounded[2 * p * GROUP : (2 * p + 2) * GROUP],
                value_buf[s, :, 2 * p * DH : 2 * (p + 1) * DH],
                preferred_element_type=jnp.float32,
            )
            for k in range(2):
                g = 2 * p + k
                block = wide[k * GROUP : (k + 1) * GROUP, k * DH : (k + 1) * DH]
                block = block * inverse[g * GROUP : (g + 1) * GROUP]
                for d in range(GROUP // own):
                    part_send[g * (GROUP // own) + d, s * own : (s + 1) * own, :] = block[
                        d * own : (d + 1) * own
                    ].astype(jnp.bfloat16)
        here = lane == me * span + s * own + lax.rem(sub, own)
        for g in range(KVH):
            level_g = jnp.where(here, level[g * GROUP : (g + 1) * GROUP], 0.0)
            stat_rows[g] = level_g if s == 0 else stat_rows[g] + level_g
        owner = jnp.where(here, request_ref[s].astype(jnp.float32), 0.0)
        owners = owner if s == 0 else owners + owner

    owners = jnp.sum(owners[:own], axis=0, keepdims=True)
    for g in range(KVH):
        for d in range(GROUP // own):
            row = jnp.sum(stat_rows[g][d * own : (d + 1) * own], axis=0, keepdims=True)
            stat_send[g * (GROUP // own) + d] = jnp.concatenate([row, owners], axis=0)

    stat_buf[me] = stat_send[me]
    part_buf[me] = part_send[me]
    for other in others:
        send(stat_send.at[other], stat_buf.at[me], 1, other)
        send(part_send.at[other], part_buf.at[me], 2, other)

    drain(new_buf.at[0], new_sem.at[0])
    drain(new_buf.at[1], new_sem.at[1])
    new_key = jnp.concatenate([new_buf[0].astype(jnp.float32)] * own, axis=0)
    new_value = jnp.concatenate([new_buf[1].astype(jnp.float32)] * own, axis=0)
    new_score = jnp.sum(mine * new_key, axis=1, keepdims=True) * scale

    drain(stat_buf.at[pl.ds(0, n - 1)], recv_sem.at[1])
    stats = jnp.sum(stat_buf[...], axis=0)
    levels = stats[0:1]
    slot_owner = stats[1:2]
    row_id = lax.broadcasted_iota(jnp.int32, (rows, n * span), 0)
    col_id = lax.broadcasted_iota(jnp.int32, (rows, n * span), 1)
    same = lax.rem(col_id, own) == lax.div(row_id, requests)
    belongs = same & (slot_owner == lax.rem(row_id, requests).astype(jnp.float32))
    peak = jnp.max(jnp.where(belongs, levels, very_negative), axis=1, keepdims=True)
    peak = jnp.maximum(peak, new_score)
    mix = jnp.where(belongs, jnp.exp2((levels - peak) * LOG2E), 0.0)
    new_weight = jnp.exp2((new_score - peak) * LOG2E)
    denom = jnp.sum(mix, axis=1, keepdims=True) + new_weight
    mix = mix * (1.0 / denom)
    new_weight = new_weight * (1.0 / denom)
    mix_high = mix.astype(jnp.bfloat16)
    mix_low = (mix - mix_high.astype(jnp.float32)).astype(jnp.bfloat16)

    drain(part_buf.at[pl.ds(0, n - 1)], recv_sem.at[2])
    parts = part_buf[...].reshape(n * span, DH)
    result = jnp.dot(
        jnp.concatenate([mix_high, mix_low], axis=0), parts, preferred_element_type=jnp.float32
    )
    result = result[:rows] + result[rows:] + new_weight * new_value
    result = jnp.concatenate(
        [result[c * requests : (c + 1) * requests] for c in range(own)], axis=1
    ).astype(jnp.bfloat16)
    out_send[...] = result
    columns = pl.ds(pl.multiple_of(me * own * DH, own * DH), own * DH)
    out_ref[:, columns] = result
    for other in others:
        send(out_send, out_ref.at[:, columns], 3, other)

    drain(q_buf.at[pl.ds(0, n - 1)], send_sem.at[0])
    drain(stat_buf.at[pl.ds(0, n - 1)], send_sem.at[1])
    drain(part_buf.at[pl.ds(0, n - 1)], send_sem.at[2])
    for k in range(per_kv):

        @pl.when(head * per_kv + k != me)
        def _():
            drain(new_buf.at[0], new_sem.at[2 + k])

    rest = out_ref.at[:, pl.ds(0, (n - 1) * own * DH)]
    drain(rest, send_sem.at[3])
    drain(rest, recv_sem.at[3])


def one_kernel(n, queries, new_kv, keys, values, slot_request, slot_length):
    requests = queries.shape[0]
    slots, block_len, width = keys.shape
    own = H // n
    span = slots * own
    bf16, f32 = jnp.bfloat16, jnp.float32
    vmem = pl.BlockSpec(memory_space=pltpu.VMEM)
    hbm = pl.BlockSpec(memory_space=pl.ANY)
    return pl.pallas_call(
        functools.partial(decode_kernel, n),
        out_shape=pltpu.VMEM((requests, H * DH), bf16),
        in_specs=[hbm] * 6,
        out_specs=vmem,
        scratch_shapes=[
            pltpu.VMEM(queries.shape, bf16),
            pltpu.VMEM(new_kv.shape, bf16),
            pltpu.SMEM(slot_request.shape, jnp.int32),
            pltpu.SMEM(slot_length.shape, jnp.int32),
            pltpu.SemaphoreType.DMA((4,)),
            pltpu.VMEM((slots, block_len, width), bf16),
            pltpu.VMEM((slots, block_len, width), bf16),
            pltpu.VMEM((own * requests, DH), bf16),
            pltpu.VMEM((n, own * requests, DH), bf16),
            pltpu.VMEM((2, requests, DH), bf16),
            pltpu.VMEM((n, span, DH), bf16),
            pltpu.VMEM((n, span, DH), bf16),
            pltpu.VMEM((n, 2, n * span), f32),
            pltpu.VMEM((n, 2, n * span), f32),
            pltpu.VMEM((requests, own * DH), bf16),
            pltpu.SemaphoreType.DMA((2 * slots,)),
            pltpu.SemaphoreType.DMA((2 + n // KVH,)),
            pltpu.SemaphoreType.DMA((4,)),
            pltpu.SemaphoreType.DMA((4,)),
        ],
        compiler_params=pltpu.CompilerParams(collective_id=0, has_side_effects=True),
    )(slot_request, slot_length, queries, new_kv, keys, values)


def joined(x, axis, combine):
    everything = jax.tree.map(lambda part: lax.all_gather(part, axis), x)
    leading = jax.tree.map(lambda part: part[0], everything)

    def turn(k, so_far):
        return combine(so_far, jax.tree.map(lambda part: part[k], everything))

    return lax.fori_loop(1, lax.axis_size(axis), turn, leading)


def combine_parts(first, second):
    top_first, sum_first, out_first = first
    top_second, sum_second, out_second = second
    peak = jnp.maximum(top_first, top_second)
    weight_first = jnp.exp(top_first - peak)
    weight_second = jnp.exp(top_second - peak)
    summed = sum_first * weight_first + sum_second * weight_second
    outputs = out_first * weight_first[..., None] + out_second * weight_second[..., None]
    return (peak, summed, outputs)


def gathered(queries, new_kv, keys, values, slot_request, slot_length):
    all_queries, all_new = (
        lax.all_gather(queries, "seq", axis=1, tiled=True),
        lax.all_gather(new_kv, "seq", axis=1, tiled=True),
    )
    requests = all_queries.shape[0]
    group_size = H // KVH
    score_scale = DH ** (-0.5)
    query_heads = all_queries.reshape(requests, KVH, group_size, DH)
    slot_count = keys.shape[0]
    block_len = keys.shape[1]
    owner = slot_request[:, None] == jnp.arange(requests, dtype=jnp.int32)[None, :]
    picked = jnp.einsum(
        "sr,rkgd->skgd", owner.astype(jnp.bfloat16), query_heads, preferred_element_type=jnp.float32
    ).astype(jnp.bfloat16)
    key_tiles = keys.reshape(slot_count, block_len, KVH, DH)
    value_tiles = values.reshape(slot_count, block_len, KVH, DH)
    scores = (
        jnp.einsum("skgd,stkd->skgt", picked, key_tiles, preferred_element_type=jnp.float32)
        * score_scale
    )
    inside = jnp.arange(block_len, dtype=jnp.int32)[None, :] < slot_length[:, None]
    scores = jnp.where(inside[:, None, None, :], scores, very_negative)
    slot_top = jnp.max(scores, axis=-1)
    weights = jnp.exp(scores - slot_top[..., None])
    slot_sum = jnp.sum(weights, axis=-1)
    slot_out = jnp.einsum(
        "skgt,stkd->skgd",
        weights.astype(jnp.bfloat16),
        value_tiles,
        preferred_element_type=jnp.float32,
    )
    owner_wide = owner[:, :, None, None]
    dense_top = jnp.max(jnp.where(owner_wide, slot_top[:, None], very_negative), axis=0)
    factor = jnp.where(owner_wide, jnp.exp(slot_top[:, None] - dense_top[None]), 0.0)
    dense_sum = jnp.sum(factor * slot_sum[:, None], axis=0)
    dense_out = jnp.einsum("srkg,skgd->rkgd", factor, slot_out, precision=lax.Precision.HIGHEST)
    total_top, total_sum, total_out = joined(
        (dense_top, dense_sum, dense_out), "seq", combine_parts
    )
    new_pair = all_new.astype(jnp.float32).reshape(requests, 2, KVH, DH)
    new_score = (
        jnp.einsum("rkgd,rkd->rkg", query_heads.astype(jnp.float32), new_pair[:, 0]) * score_scale
    )
    peak = jnp.maximum(total_top, new_score)
    old_weight = jnp.exp(total_top - peak)
    new_weight = jnp.exp(new_score - peak)
    rounded_new = new_weight.astype(jnp.bfloat16).astype(jnp.float32)
    numer = (
        total_out * old_weight[..., None] + rounded_new[..., None] * new_pair[:, 1][:, :, None, :]
    )
    denom = total_sum * old_weight + new_weight
    attended = numer / denom[..., None]
    return attended.reshape(requests, H * DH).astype(jnp.bfloat16)


def shards(n, queries, new_kv, keys, values, slot_request, slot_length):
    whole_heads = n == 2 * KVH and n * keys.shape[0] * (H // n) == DH
    if whole_heads:
        return one_kernel(n, queries, new_kv, keys, values, slot_request, slot_length)
    return gathered(queries, new_kv, keys, values, slot_request, slot_length)


def solution(mesh):
    placed = (
        P("parts", "seq"),
        P("parts", "seq"),
        P(("parts", "seq"), None, None),
        P(("parts", "seq"), None, None),
        P(("parts", "seq")),
        P(("parts", "seq")),
    )
    return jax.shard_map(
        functools.partial(shards, mesh.shape["seq"]),
        mesh=mesh,
        in_specs=placed,
        out_specs=P("parts", None),
        check_vma=False,
    )
```
